128 devices in a mesh: expert: 8 (over z_lo, x), shard: 16 (over z_hi, y, core).
Axes of the slice: x: 4, y: 4, z: 4 (z_hi: 2, z_lo: 2; z = z_hi * 2 + z_lo), core: 2. Of those that a mesh axis runs over, the one named last changes fastest.
Arguments:
- master_gate: float32 [128, 2048, 768], P('expert', 'shard'), may hold values from -0.1875 to 0.1875
- master_up: float32 [128, 2048, 768], P('expert', 'shard'), may hold values from -0.1875 to 0.1875
- router_weight: float32 [2048, 128], P('shard', 'expert'), may hold values from -0.125 to 0.125
- router_gain: float32 [2048], P('shard'), may hold values from 0.25 to 1.75
Outputs:
- final_gate: bfloat16 [128, 2048, 768], P(('expert', 'shard'))
- final_up: bfloat16 [128, 2048, 768], P(('expert', 'shard'))
- scale_gate: float32 [128, 768], P(('expert', 'shard'))
- scale_up: float32 [128, 768], P(('expert', 'shard'))
- serve_router: bfloat16 [2048, 128], replicated
The draws below stay inside these ranges and needn't reach their ends.
All inputs are finite; a program needn't handle non-finite values. Where the reference program divides by a largest or mean magnitude, that divisor is 1e-20 or more.
Results may differ from the reference program's by a relative error of at most 0.001.
Values may be sent and summed in bfloat16 or wider, within the bound.
No kernel may reach another device: no remote copies, remote signals or barrier semaphores. Data moves between devices by JAX's collectives and lax.ppermute only.
A program may use at most 128 MiB of HBM per device.

```python
import jax
import jax.numpy as jnp

EXPERTS = 128
D_MODEL = 2048
D_EXPERT = 768


def spiked(array, key, source, target, parts, factor):
    def block_of(dim):
        return (jnp.arange(array.shape[dim]) // (array.shape[dim] // parts)).reshape((-1,) + (1,) * (array.ndim - 1 - dim))

    one_side = jax.random.permutation(key, parts)[block_of(target)]
    other_side = (block_of(target) + parts // 2) % parts
    return jnp.where((block_of(source) == one_side) | (block_of(source) == other_side), factor * array, array)


def shard_levels(own_key, extent, split, low, largest):
    loudness, own = 1.0, jax.random.fold_in(own_key, 6)
    for position, shards_of in split:
        heights = jnp.exp(jax.random.uniform(jax.random.fold_in(own, position), (shards_of,), jnp.float32, low / len(split), largest / len(split)))
        loudness = loudness * jnp.repeat(heights, extent[position] // shards_of).reshape([-1 if axis == position else 1 for axis in range(len(extent))])
    return loudness


def gaussian(rng, shape, spread, most, cuts=(), held_as=jnp.bfloat16):
    gain = shard_levels(rng, shape, cuts, -0.22, 0.18) if cuts else 1.0
    array = jax.random.normal(rng, shape, jnp.float32) * spread * gain
    return jnp.minimum(jnp.maximum(array, -most), most).astype(held_as)


def gaussian_with(own_key, dims, deviation, bound, cuts, heavy, kind=jnp.bfloat16):
    array = deviation * jax.random.normal(own_key, dims, jnp.float32)
    if cuts:
        array = array * shard_levels(own_key, dims, cuts, -0.22, 0.18)
    return jnp.clip(spiked(array, jax.random.fold_in(own_key, 3), *heavy), -bound, bound).astype(kind)


def setup_inputs(seed: int = 0) -> dict:
    streams_of = jax.random.split(jax.random.key(seed), 5)
    return {
        "master_gate": gaussian_with(streams_of[0], (EXPERTS, D_MODEL, D_EXPERT), D_MODEL ** -0.5, 0.1875, ((0, 8), (1, 16)), (1, 2, 16, 2.0), jnp.float32),
        "master_up": gaussian_with(streams_of[1], (EXPERTS, D_MODEL, D_EXPERT), D_MODEL ** -0.5, 0.1875, ((0, 8), (1, 16)), (1, 2, 16, 2.0), jnp.float32),
        "router_weight": gaussian(streams_of[2], (D_MODEL, EXPERTS), D_MODEL ** -0.5, 0.125, ((0, 16), (1, 8)), jnp.float32),
        "router_gain": jnp.clip(1.0 + 0.15 * jax.random.normal(streams_of[3], (D_MODEL,), jnp.float32), 0.25, 1.75),
    }


def reference(master_gate, master_up, router_weight, router_gain):
    scale_gate = jnp.sum(jnp.abs(master_gate), axis=1) / D_MODEL
    final_gate = (master_gate / jnp.expand_dims(scale_gate, 1)).astype(jnp.bfloat16)
    scale_up = jnp.sum(jnp.abs(master_up), axis=1) / D_MODEL
    final_up = (master_up / jnp.expand_dims(scale_up, 1)).astype(jnp.bfloat16)
    serve_router = (router_weight * router_gain[:, None]).astype(jnp.bfloat16)
    return final_gate, final_up, scale_gate, scale_up, serve_router
```

```python
import functools

import jax
import jax.numpy as jnp
from jax import lax
from jax.experimental import pallas as pl
from jax.experimental.pallas import tpu as pltpu
from jax.sharding import Mesh
from jax.sharding import PartitionSpec as P


SHARD = ("zh", "y", "c")
ALL = ("zl", "x", "zh", "y", "c")
ROWS, COLS, HALF, LANES = 128, 768, 6, 128
TILES = 2 * HALF
BODY = TILES * ROWS
MSG = BODY + 16
SPAN, LOW = 250.0, 125.0
D_MODEL = 2048

ORDER = [
    (1, 0, 0), (0, 1, 0), (0, 3, 0), (1, 1, 0), (0, 2, 0), (1, 3, 0), (1, 2, 0),
    (1, 0, 1), (0, 1, 1), (0, 3, 1), (1, 1, 1), (0, 2, 1), (1, 3, 1), (1, 2, 1),
    (0, 0, 1), (0, 0, 0),
]
FIRST = 4


def encode_kernel(n, dst, gate, up, *refs):
    msgs, sums, buf, sems = refs[:n], refs[n], refs[n + 1], refs[n + 2]
    copies = []
    for k in range(n):
        for h, src in enumerate((gate, up)):
            copies.append(pltpu.make_async_copy(src.at[dst[k]], buf.at[k, h], sems.at[k, h]))
    for c in copies:
        c.start()
    for k in range(n):
        for h in range(2):
            copies[2 * k + h].wait()
            for i in range(HALF):
                j = h * HALF + i
                v = buf[k, h, :, i * LANES : (i + 1) * LANES]
                a = jnp.abs(v)
                sums[k, j : j + 1, :] = jnp.sum(a, axis=0, keepdims=True)
                top = jnp.max(a, axis=0, keepdims=True)
                unit = jnp.maximum(top * 1.01, 1e-30).astype(jnp.bfloat16)
                msgs[k][BODY + j : BODY + j + 1, :] = unit
                y = jnp.exp2(a * (SPAN / unit.astype(jnp.float32)) - LOW)
                msgs[k][j * ROWS : (j + 1) * ROWS, :] = jnp.where(v < 0, -y, y).astype(jnp.bfloat16)
        msgs[k][BODY + TILES : MSG, :] = jnp.zeros((MSG - BODY - TILES, LANES), jnp.bfloat16)


def encode(dst, gate, up):
    n = dst.shape[0]
    vmem = pl.BlockSpec(memory_space=pltpu.VMEM)
    out = pl.pallas_call(
        functools.partial(encode_kernel, n),
        in_specs=[pl.BlockSpec(memory_space=pltpu.SMEM)] + [pl.BlockSpec(memory_space=pl.ANY)] * 2,
        out_specs=[vmem] * (n + 1),
        out_shape=[jax.ShapeDtypeStruct((MSG, LANES), jnp.bfloat16)] * n
        + [jax.ShapeDtypeStruct((n, TILES, LANES), jnp.float32)],
        scratch_shapes=[pltpu.VMEM((n, 2, ROWS, COLS), jnp.float32), pltpu.SemaphoreType.DMA((n, 2))],
        name="encode",
    )(dst, gate, up)
    return out[:n], out[n]


def decode_kernel(n, chained, src, total, *refs):
    msgs, refs = refs[:n], refs[n + (2 if chained else 0) :]
    outs, buf, sems = refs[:2], refs[2], refs[3]
    copies = []
    for k in range(n):
        for h in range(2):
            for i in range(HALF):
                j = h * HALF + i
                unit = msgs[k][BODY + j : BODY + j + 1, :].astype(jnp.float32)
                gain = unit * (D_MODEL / SPAN) / total[j : j + 1, :]
                v = msgs[k][j * ROWS : (j + 1) * ROWS, :].astype(jnp.float32)
                w = (jnp.log2(jnp.abs(v)) + LOW) * gain
                buf[k, h, :, i * LANES : (i + 1) * LANES] = jnp.where(v < 0, -w, w).astype(jnp.bfloat16)
            rows = pl.ds(pl.multiple_of(src[k] * ROWS, ROWS), ROWS)
            c = pltpu.make_async_copy(buf.at[k, h], outs[h].at[0, rows, :], sems.at[k, h])
            c.start()
            copies.append(c)
    for c in copies:
        c.wait()


def decode(src, total, msgs, outs):
    n, chained = len(msgs), outs is not None
    vmem, hbm = pl.BlockSpec(memory_space=pltpu.VMEM), pl.BlockSpec(memory_space=pl.ANY)
    shape = jax.ShapeDtypeStruct((1, D_MODEL, COLS), jnp.bfloat16)
    return pl.pallas_call(
        functools.partial(decode_kernel, n, chained),
        in_specs=[pl.BlockSpec(memory_space=pltpu.SMEM), vmem] + [vmem] * n + [hbm] * (2 if chained else 0),
        out_specs=[hbm] * 2,
        out_shape=[shape] * 2,
        input_output_aliases={2 + n: 0, 3 + n: 1} if chained else {},
        scratch_shapes=[pltpu.VMEM((n, 2, ROWS, COLS), jnp.bfloat16), pltpu.SemaphoreType.DMA((n, 2))],
        name="decode",
    )(src, total, *msgs, *(outs if chained else ()))


def router_kernel(rows, cols, parts, out, buf):
    for q in range(4):
        for p in range(16):
            for b in range(2):
                at = pl.multiple_of(cols[2 * q + b] * 16, 16)
                buf[rows[p], pl.ds(at, 16), :] = parts[q, b, p].astype(jnp.float32)
    for s in range(16):
        out[s * ROWS : (s + 1) * ROWS, :] = buf[s].T.astype(jnp.bfloat16)


def arrange_router(rows, cols, parts):
    smem, vmem = pl.BlockSpec(memory_space=pltpu.SMEM), pl.BlockSpec(memory_space=pltpu.VMEM)
    return pl.pallas_call(
        router_kernel,
        in_specs=[smem, smem, vmem],
        out_specs=vmem,
        out_shape=jax.ShapeDtypeStruct((D_MODEL, 128), jnp.bfloat16),
        scratch_shapes=[pltpu.VMEM((16, 128, LANES), jnp.float32)],
        name="router",
    )(rows, cols, parts)


def moves(dz, dy, dc):
    return [
        (z * 8 + y * 2 + c, (z ^ dz) * 8 + ((y + dy) % 4) * 2 + (c ^ dc))
        for z in range(2) for y in range(4) for c in range(2)
    ]


def send(value, dz, dy, dc):
    return lax.ppermute(value, SHARD, moves(dz, dy, dc))


def body(gate, up, weight, gain):
    zl, x, zh, y, c = (lax.axis_index(a) for a in ALL)
    index = lambda dz, dy, dc: (zh ^ dz) * 8 + ((y + dy) % 4) * 2 + (c ^ dc)
    dst = [index(*o) for o in ORDER]
    src = [index(dz, -dy, dc) for dz, dy, dc in ORDER]

    first, sums_a = encode(jnp.stack(dst[:FIRST]), gate, up)
    got = {o: send(m, *o) for o, m in zip(ORDER[:FIRST], first)}
    rest, sums_b = encode(jnp.stack(dst[FIRST:]), gate, up)

    sums = {o: (sums_a[k] if k < FIRST else sums_b[k - FIRST]) for k, o in enumerate(ORDER)}
    router = (weight * gain[:, None]).astype(jnp.bfloat16).astype(jnp.float32).T

    ys, cs = (0, 1, 2, 3), (0, 1)
    got_z = send(jnp.concatenate([sums[1, dy, dc] for dy in ys for dc in cs] + [router], axis=0), 1, 0, 0)
    for o, m in zip(ORDER[FIRST:8], rest):
        got[o] = send(m, *o)
    half = jnp.stack([sums[0, dy, dc] for dy in ys for dc in cs]) + got_z[: 8 * TILES].reshape(8, TILES, LANES)
    pair = jnp.concatenate([router, got_z[8 * TILES :]], axis=0)
    got_y = [send(jnp.concatenate([half[2 * dy], half[2 * dy + 1], pair], axis=0), 0, dy, 0) for dy in (1, 2, 3)]
    for o, m in zip(ORDER[8:12], rest[8 - FIRST :]):
        got[o] = send(m, *o)
    quarter = half[:2]
    for g in got_y:
        quarter = quarter + g[: 2 * TILES].reshape(2, TILES, LANES)
    octet = jnp.concatenate([pair] + [g[2 * TILES :] for g in got_y], axis=0)
    got_c = send(jnp.concatenate([quarter[1], octet], axis=0), 0, 0, 1)
    for o, m in zip(ORDER[12:15], rest[12 - FIRST :]):
        got[o] = send(m, *o)
    total = quarter[0] + got_c[:TILES]
    both = jnp.concatenate([octet, got_c[TILES:]], axis=0).astype(jnp.bfloat16)
    other = lax.ppermute(both, "zl", [(0, 1), (1, 0)])
    mine = jnp.stack([both, other])
    others = [lax.ppermute(mine, "x", [(i, (i + d) % 4) for i in range(4)]) for d in (1, 2, 3)]
    parts = jnp.stack([mine] + others).reshape(4, 2, 16, 16, LANES)
    rows = jnp.stack([index(dz, -dy, dc) for dc in cs for dy in ys for dz in (0, 1)])
    cols = jnp.stack([(zl ^ b) * 4 + (x - d) % 4 for d in range(4) for b in (0, 1)])
    serve_router = arrange_router(rows, cols, parts)

    got[0, 0, 0] = rest[-1]
    scale = (total / D_MODEL).reshape(1, 2 * COLS)
    outs = None
    order = [15] + list(range(15))
    for group in (order[:4], order[4:7], order[7:10], order[10:12], order[12:14], order[14:]):
        outs = decode(jnp.stack([src[k] for k in group]), total, [got[ORDER[k]] for k in group], outs)
    return outs[0], outs[1], scale[:, :COLS], scale[:, COLS:], serve_router


def solution(mesh):
    finer = Mesh(mesh.devices.reshape(2, 4, 2, 4, 2), ALL)
    expert = ("zl", "x")
    in_specs = (P(expert, SHARD, None), P(expert, SHARD, None), P(SHARD, expert), P(SHARD))
    out_specs = (P(ALL, None, None), P(ALL, None, None), P(ALL, None), P(ALL, None), P())
    return jax.shard_map(body, mesh=finer, in_specs=in_specs, out_specs=out_specs, check_vma=False)
```

```python
import functools

import jax
import jax.numpy as jnp
from jax import lax
from jax.experimental import pallas as pl
from jax.experimental.pallas import tpu as pltpu
from jax.sharding import Mesh
from jax.sharding import PartitionSpec as P


SHARD = ("zh", "y", "c")
ALL = ("zl", "x", "zh", "y", "c")
D_MODEL, ROWS, COLS, LANES, HALF = 2048, 128, 768, 128, 6
TILES = 2 * HALF
BODY = TILES * ROWS
TAIL = BODY + 16
SPAN, LOW = 250.0, 125.0
GRANT = 16 * 2**20
BF16, F32 = jnp.bfloat16, jnp.float32

PRE = [(0, 1, 1), (0, 3, 1), (1, 0, 0)]
MID = [(1, 1, 0), (0, 3, 0)]
MAIN = [(1, 2, 0), (1, 3, 0), (1, 0, 1), (1, 1, 1), (1, 3, 1), (1, 2, 1)]
MORE = [(0, 1, 0), (0, 2, 0), (0, 2, 1), (0, 0, 1), (0, 0, 0)]

VMEM = pl.BlockSpec(memory_space=pltpu.VMEM)
HBM = pl.BlockSpec(memory_space=pl.ANY)


def where_am_i():
    return tuple(lax.axis_index(a) for a in SHARD)


def index(here, dz, dy, dc):
    zh, y, c = here
    return (zh ^ dz) * 8 + ((y + dy) % 4) * 2 + (c ^ dc)


def at(o):
    return o[1] * 2 + o[2]


def fetch(here, gate, up, offsets, buf, sems):
    copies = []
    for k, o in enumerate(offsets):
        d = index(here, *o)
        copies.append([pltpu.make_async_copy(a.at[d], buf.at[k, h], sems.at[k, h]) for h, a in enumerate((gate, up))])
    for pair in copies:
        for c in pair:
            c.start()
    return copies


def encode_block(copies, buf, k, msg, put_sum):
    for h in range(2):
        copies[k][h].wait()
        units = []
        for i in range(HALF):
            a = jnp.abs(buf[k, h, :, i * LANES : (i + 1) * LANES])
            put_sum(h * HALF + i, jnp.sum(a, axis=0, keepdims=True))
            units.append(jnp.maximum(jnp.max(a, axis=0, keepdims=True) * 1.01, 1e-30).astype(BF16))
        if msg is None:
            continue
        for i, unit in enumerate(units):
            j = h * HALF + i
            msg[BODY + j : BODY + j + 1, :] = unit
            v = buf[k, h, :, i * LANES : (i + 1) * LANES]
            y = jnp.exp2(jnp.abs(v) * (SPAN / unit.astype(F32)) - LOW)
            msg[j * ROWS : (j + 1) * ROWS, :] = jnp.where(v < 0, -y, y).astype(BF16)


def into(ref, base, step, q):
    def put(j, row):
        ref[base + j * step + q : base + j * step + q + 1, :] = row
    return put


def split(s):
    hi = s.astype(BF16)
    return hi, (s - hi.astype(F32)).astype(BF16)


def joined(ref, base, n):
    return ref[base : base + n, :].astype(F32) + ref[base + n : base + 2 * n, :].astype(F32)


def pre_kernel(gate, up, weight, gain, *refs):
    n = len(PRE)
    msgs, sums, router, buf, wbuf, gbuf, sems, wsems = refs[:n], *refs[n:]
    copies = fetch(where_am_i(), gate, up, PRE, buf, sems)
    small = [pltpu.make_async_copy(weight, wbuf, wsems.at[0]), pltpu.make_async_copy(gain, gbuf, wsems.at[1])]
    for c in small:
        c.start()
    sums[...] = jnp.zeros_like(sums)
    for k, o in enumerate(PRE):
        encode_block(copies, buf, k, msgs[k], into(sums, o[0] * 96, 8, at(o)))
    for c in small:
        c.wait()
    router[...] = (wbuf[...] * gbuf[...]).astype(BF16)


def mid_kernel(gate, up, sums_in, *refs):
    n = len(MID)
    msgs, sums, buf, sems = refs[:n], *refs[n:]
    copies = fetch(where_am_i(), gate, up, MID, buf, sems)
    sums[...] = sums_in[...]
    for k, o in enumerate(MID):
        encode_block(copies, buf, k, msgs[k], into(sums, o[0] * 96, 8, at(o)))


def main_kernel(gate, up, sums_in, router, other, *refs):
    n = len(MAIN)
    msgs, sums, note, buf, sems = refs[:n], *refs[n:]
    copies = fetch(where_am_i(), gate, up, MAIN, buf, sems)
    sums[...] = sums_in[...]
    for k, o in enumerate(MAIN):
        encode_block(copies, buf, k, msgs[k], into(sums, o[0] * 96, 8, at(o)))
    hi, lo = split(sums[96:192, :])
    note[0:96, :] = hi
    note[96:192, :] = lo
    note[192:208, :] = router[...]
    note[208:224, :] = other[...]


def more_kernel(gate, up, sums_in, *refs):
    n = len(MORE)
    msgs, sums, buf, sems = refs[: n - 1], *refs[n - 1 :]
    copies = fetch(where_am_i(), gate, up, MORE, buf, sems)
    sums[...] = sums_in[0:96, :]
    for k, o in enumerate(MORE):
        encode_block(copies, buf, k, msgs[k] if k < n - 1 else None, into(sums, 0, 8, at(o)))


def y_kernel(sums, note, got, *refs):
    notes, half, pair, stage = refs[:3], *refs[3:]
    half[...] = sums[...] + joined(got, 0, 96)
    pair[0:32, :] = note[192:224, :]
    pair[32:64, :] = got[192:224, :]
    stage[...] = jnp.zeros_like(stage)
    for k in range(3):
        for dc in range(2):
            for j in range(TILES):
                q = j * 8 + 2 * (k + 1) + dc
                stage[dc * 16 + j : dc * 16 + j + 1, :] = half[q : q + 1, :]
        hi, lo = split(stage[...])
        notes[k][0:32, :] = hi
        notes[k][32:64, :] = lo
        notes[k][64:128, :] = pair[...]


def c_kernel(half, pair, got1, got2, got3, m0, msg, quarter, octet):
    quarter[...] = joined(got1, 0, 32) + joined(got2, 0, 32) + joined(got3, 0, 32)
    octet[0:64, :] = pair[...]
    for dy, g in ((1, got1), (2, got2), (3, got3)):
        octet[dy * 64 : dy * 64 + 64, :] = g[64:128, :]
    for dc in range(2):
        for j in range(TILES):
            r, q = dc * 16 + j, j * 8 + dc
            quarter[r : r + 1, :] = quarter[r : r + 1, :] + half[q : q + 1, :]
    hi, lo = split(quarter[16:32, :])
    msg[TAIL : TAIL + 16, :] = hi
    msg[TAIL + 16 : TAIL + 32, :] = lo
    msg[TAIL + 32 : TAIL + 288, :] = octet[...]


def total_kernel(gate, up, quarter, octet, got, out_g, out_u, total, sg, su, board, buf, obuf, sems, osems):
    here = where_am_i()
    copies = fetch(here, gate, up, [(0, 0, 0)], buf, sems)
    total[...] = quarter[0:16, :] + joined(got, TAIL, 16)
    board[0:256, :] = octet[...]
    board[256:512, :] = got[TAIL + 32 : TAIL + 288, :]
    for i in range(HALF):
        sg[0:1, i * LANES : (i + 1) * LANES] = total[i : i + 1, :] / D_MODEL
        su[0:1, i * LANES : (i + 1) * LANES] = total[HALF + i : HALF + i + 1, :] / D_MODEL
    rows = pl.ds(pl.multiple_of(index(here, 0, 0, 0) * ROWS, ROWS), ROWS)
    back = []
    for h, out in enumerate((out_g, out_u)):
        copies[0][h].wait()
        for i in range(HALF):
            gain = D_MODEL / total[h * HALF + i : h * HALF + i + 1, :]
            cols = slice(i * LANES, (i + 1) * LANES)
            obuf[h, :, cols] = (buf[0, h, :, cols] * gain).astype(BF16)
        back.append(pltpu.make_async_copy(obuf.at[h], out.at[0, rows, :], osems.at[h]))
        back[-1].start()
    for b in back:
        b.wait()


def decode_kernel(offsets, total, *refs):
    n = len(offsets)
    msgs, outs, (buf, sems) = refs[:n], refs[n + 2 : n + 4], refs[n + 4 :]
    here = where_am_i()
    copies = []
    for k, (dz, dy, dc) in enumerate(offsets):
        rows = pl.ds(pl.multiple_of(index(here, dz, 4 - dy, dc) * ROWS, ROWS), ROWS)
        for h in range(2):
            for i in range(HALF):
                j = h * HALF + i
                unit = msgs[k][BODY + j : BODY + j + 1, :].astype(F32)
                gain = unit * (D_MODEL / SPAN) / total[j : j + 1, :]
                v = msgs[k][j * ROWS : (j + 1) * ROWS, :].astype(F32)
                w = (jnp.log2(jnp.abs(v)) + LOW) * gain
                buf[k, h, :, i * LANES : (i + 1) * LANES] = jnp.where(v < 0, -w, w).astype(BF16)
            copies.append(pltpu.make_async_copy(buf.at[k, h], outs[h].at[0, rows, :], sems.at[k, h]))
            copies[-1].start()
    for c in copies:
        c.wait()


def router_kernel(*refs):
    boards, out, buf = refs[:4], refs[4], refs[5]
    here = where_am_i()
    zl, x = lax.axis_index("zl"), lax.axis_index("x")
    for d in range(4):
        for b in range(2):
            col = pl.multiple_of(((zl ^ b) * 4 + (x + 8 - d - b) % 4) * 16, 16)
            for p in range(16):
                dc, dy, dz = p // 8, (p // 2) % 4, p % 2
                piece = boards[d][p * 32 + b * 16 : p * 32 + b * 16 + 16, :]
                buf[index(here, dz, 4 - dy, dc), pl.ds(col, 16), :] = piece.astype(F32)
    for s in range(16):
        out[s * ROWS : (s + 1) * ROWS, :] = buf[s].T.astype(BF16)


def shape(*dims, dtype=BF16):
    return jax.ShapeDtypeStruct(dims, dtype)


def local(*dims, dtype=BF16):
    return pltpu.VMEM(dims, dtype)


def message(extra=0):
    return local(TAIL + extra, LANES)


def near(value):
    return pltpu.with_memory_space_constraint(value, pltpu.VMEM)


def far(value):
    return pltpu.with_memory_space_constraint(value, pltpu.HBM)


def blocks(n):
    return [pltpu.VMEM((n, 2, ROWS, COLS), F32), pltpu.SemaphoreType.DMA((n, 2))]


def call(kernel, ins, outs, out_specs=None, **kw):
    def run(*args):
        return pl.pallas_call(
            kernel, in_specs=ins, out_specs=out_specs or [VMEM] * len(outs), out_shape=outs,
            compiler_params=pltpu.CompilerParams(vmem_limit_bytes=GRANT), **kw
        )(*args)
    return run


def moves(dz, dy, dc):
    return [
        (z * 8 + y * 2 + c, (z ^ dz) * 8 + ((y + dy) % 4) * 2 + (c ^ dc))
        for z in range(2) for y in range(4) for c in range(2)
    ]


def send(value, o):
    return lax.ppermute(value, SHARD, moves(*o))


GROUPS = [
    [(1, 0, 0), (0, 1, 1), (0, 3, 1), (1, 1, 0), (0, 3, 0), (1, 2, 0)],
    [(0, 1, 0), (1, 3, 0), (0, 2, 0), (0, 0, 1)],
    [(1, 0, 1), (1, 1, 1)],
    [(0, 2, 1), (1, 3, 1)],
    [(1, 2, 1)],
]


def step(gate, up, weight, gain):
    got = {}
    gate, up, weight, gain = (far(v) for v in (gate, up, weight.T, gain[None]))
    *first, sums, router = call(
        pre_kernel, [HBM] * 4, [message()] * len(PRE) + [local(192, LANES, dtype=F32), local(16, LANES)],
        scratch_shapes=[blocks(len(PRE))[0], pltpu.VMEM((16, LANES), F32), pltpu.VMEM((1, LANES), F32),
                        blocks(len(PRE))[1], pltpu.SemaphoreType.DMA((2,))],
    )(gate, up, weight, gain)
    for o, m in zip(PRE, first):
        got[o] = send(m, o)
    turn = [(z * 4 + x, (1 - z) * 4 + (x + 1) % 4) for z in range(2) for x in range(4)]
    other = near(lax.ppermute(router, ("zl", "x"), turn))
    *early, sums = call(
        mid_kernel, [HBM] * 2 + [VMEM], [message()] * len(MID) + [local(192, LANES, dtype=F32)],
        scratch_shapes=blocks(len(MID)),
    )(gate, up, sums)
    for o, m in zip(MID, early):
        got[o] = send(m, o)
    *rest, sums, note = call(
        main_kernel, [HBM] * 2 + [VMEM] * 3,
        [message()] * len(MAIN) + [local(192, LANES, dtype=F32), local(224, LANES)], scratch_shapes=blocks(len(MAIN)),
    )(gate, up, sums, router, other)
    turn = [(x * 2 + z, (x + 1) % 4 * 2 + 1 - z) for x in range(4) for z in range(2)]
    passed = near(lax.ppermute(note, ("x", "zh"), turn))
    got_note = near(lax.ppermute(passed, "x", [(i, (i + 3) % 4) for i in range(4)]))
    for o, m in zip(MAIN, rest):
        got[o] = send(m, o)
    *last, sums = call(
        more_kernel, [HBM] * 2 + [VMEM],
        [message()] * 3 + [message(288), local(96, LANES, dtype=F32)], scratch_shapes=blocks(len(MORE)),
    )(gate, up, sums)
    for o, m in zip(MORE[:3], last):
        got[o] = send(m, o)
    *notes, half, pair = call(
        y_kernel, [VMEM] * 3, [local(128, LANES)] * 3 + [local(96, LANES, dtype=F32), local(64, LANES)],
        scratch_shapes=[pltpu.VMEM((32, LANES), F32)],
    )(sums, note, got_note)
    got_y = []
    for dy, v in zip((1, 2, 3), notes):
        got_y.append(near(lax.ppermute(v, SHARD, moves(0, dy, 0))))
    across, quarter, octet = call(
        c_kernel, [VMEM] * 6, [message(288), local(32, LANES, dtype=F32), local(256, LANES)],
        input_output_aliases={5: 0},
    )(half, pair, *got_y, last[3])
    got[0, 0, 1] = near(send(across, (0, 0, 1)))
    whole = shape(1, D_MODEL, COLS)
    *outs, total, scale_gate, scale_up, board = call(
        total_kernel, [HBM] * 2 + [VMEM] * 3,
        [whole, whole, local(16, LANES, dtype=F32), shape(1, COLS, dtype=F32), shape(1, COLS, dtype=F32), local(512, LANES)],
        [HBM] * 2 + [VMEM] * 4,
        scratch_shapes=[blocks(1)[0], pltpu.VMEM((2, ROWS, COLS), BF16), blocks(1)[1], pltpu.SemaphoreType.DMA((2,))],
    )(gate, up, quarter, octet, got[0, 0, 1])
    boards = [board]
    for d in (1, 2, 3):
        boards.append(near(lax.ppermute(board, "x", [(i, (i + d) % 4) for i in range(4)])))
    for offsets in GROUPS:
        n = len(offsets)
        outs = call(
            functools.partial(decode_kernel, offsets), [VMEM] * (n + 1) + [HBM] * 2, [whole] * 2, [HBM] * 2,
            input_output_aliases={n + 1: 0, n + 2: 1},
            scratch_shapes=[pltpu.VMEM((n, 2, ROWS, COLS), BF16), pltpu.SemaphoreType.DMA((n, 2))],
        )(total, *(near(got[o]) for o in offsets), *outs)
    (serve_router,) = call(
        router_kernel, [VMEM] * 4, [shape(D_MODEL, LANES)], scratch_shapes=[pltpu.VMEM((16, LANES, LANES), F32)]
    )(*boards)
    return outs[0], outs[1], scale_gate, scale_up, serve_router


def solution(mesh):
    finer = Mesh(mesh.devices.reshape(2, 4, 2, 4, 2), ALL)
    expert = ("zl", "x")
    in_specs = (P(expert, SHARD, None), P(expert, SHARD, None), P(SHARD, expert), P(SHARD))
    out_specs = (P(ALL, None, None), P(ALL, None, None), P(ALL, None), P(ALL, None), P())
    return jax.shard_map(step, mesh=finer, in_specs=in_specs, out_specs=out_specs, check_vma=False)
```

```python
import functools

import jax
import jax.numpy as jnp
from jax import lax
from jax.experimental import pallas as pl
from jax.experimental.pallas import tpu as pltpu
from jax.sharding import Mesh
from jax.sharding import PartitionSpec as P


SHARD = ("zh", "y", "c")
ALL = ("zl", "x", "zh", "y", "c")
D_MODEL, ROWS, COLS, LANES, HALF = 2048, 128, 768, 128, 6
TILES = 2 * HALF
BODY = TILES * ROWS
TAIL = BODY + 16
SPAN, LOW = 250.0, 125.0
GRANT = 16 * 2**20
BF16, F32 = jnp.bfloat16, jnp.float32

PRE = [(0, 1, 1), (0, 3, 1), (1, 0, 0)]
MID = [(1, 1, 0), (0, 3, 0)]
MAIN = [(1, 2, 0), (1, 3, 0), (1, 0, 1), (1, 1, 1), (1, 3, 1), (1, 2, 1)]
MORE = [(0, 1, 0), (0, 2, 0), (0, 2, 1), (0, 0, 1), (0, 0, 0)]

VMEM = pl.BlockSpec(memory_space=pltpu.VMEM)
HBM = pl.BlockSpec(memory_space=pl.ANY)


def where_am_i():
    return tuple(lax.axis_index(a) for a in SHARD)


def index(here, dz, dy, dc):
    zh, y, c = here
    return (zh ^ dz) * 8 + ((y + dy) % 4) * 2 + (c ^ dc)


def at(o):
    return o[1] * 2 + o[2]


def fetch(here, gate, up, offsets, buf, sems):
    copies = []
    for k, o in enumerate(offsets):
        d = index(here, *o)
        copies.append([pltpu.make_async_copy(a.at[d], buf.at[k, h], sems.at[k, h]) for h, a in enumerate((gate, up))])
    for pair in copies:
        for c in pair:
            c.start()
    return copies


def encode_block(copies, buf, k, msg, put_sum):
    for h in range(2):
        copies[k][h].wait()
        units = []
        for i in range(HALF):
            a = jnp.abs(buf[k, h, :, i * LANES : (i + 1) * LANES])
            put_sum(h * HALF + i, jnp.sum(a, axis=0, keepdims=True))
            units.append(jnp.maximum(jnp.max(a, axis=0, keepdims=True) * 1.01, 1e-30).astype(BF16))
        if msg is None:
            continue
        for i, unit in enumerate(units):
            j = h * HALF + i
            msg[BODY + j : BODY + j + 1, :] = unit
            v = buf[k, h, :, i * LANES : (i + 1) * LANES]
            y = jnp.exp2(jnp.abs(v) * (SPAN / unit.astype(F32)) - LOW)
            msg[j * ROWS : (j + 1) * ROWS, :] = jnp.where(v < 0, -y, y).astype(BF16)


def into(ref, base, step, q):
    def put(j, row):
        ref[base + j * step + q : base + j * step + q + 1, :] = row
    return put


def split(s):
    hi = s.astype(BF16)
    return hi, (s - hi.astype(F32)).astype(BF16)


def joined(ref, base, n):
    return ref[base : base + n, :].astype(F32) + ref[base + n : base + 2 * n, :].astype(F32)


def pre_kernel(gate, up, weight, gain, *refs):
    n = len(PRE)
    msgs, sums, router, buf, wbuf, gbuf, sems, wsems = refs[:n], *refs[n:]
    copies = fetch(where_am_i(), gate, up, PRE, buf, sems)
    small = [pltpu.make_async_copy(weight, wbuf, wsems.at[0]), pltpu.make_async_copy(gain, gbuf, wsems.at[1])]
    for c in small:
        c.start()
    sums[...] = jnp.zeros_like(sums)
    for k, o in enumerate(PRE):
        encode_block(copies, buf, k, msgs[k], into(sums, o[0] * 96, 8, at(o)))
    for c in small:
        c.wait()
    router[...] = (wbuf[...] * gbuf[...]).astype(BF16)


def mid_kernel(gate, up, sums_in, *refs):
    n = len(MID)
    msgs, sums, buf, sems = refs[:n], *refs[n:]
    copies = fetch(where_am_i(), gate, up, MID, buf, sems)
    sums[...] = sums_in[...]
    for k, o in enumerate(MID):
        encode_block(copies, buf, k, msgs[k], into(sums, o[0] * 96, 8, at(o)))


def main_kernel(gate, up, sums_in, router, other, *refs):
    n = len(MAIN)
    msgs, sums, note, buf, sems = refs[:n], *refs[n:]
    copies = fetch(where_am_i(), gate, up, MAIN, buf, sems)
    sums[...] = sums_in[...]
    for k, o in enumerate(MAIN):
        encode_block(copies, buf, k, msgs[k], into(sums, o[0] * 96, 8, at(o)))
    hi, lo = split(sums[96:192, :])
    note[0:96, :] = hi
    note[96:192, :] = lo
    note[192:208, :] = router[...]
    note[208:224, :] = other[...]


def more_kernel(gate, up, sums_in, *refs):
    n = len(MORE)
    msgs, sums, buf, sems = refs[: n - 1], *refs[n - 1 :]
    copies = fetch(where_am_i(), gate, up, MORE, buf, sems)
    sums[...] = sums_in[0:96, :]
    for k, o in enumerate(MORE):
        encode_block(copies, buf, k, msgs[k] if k < n - 1 else None, into(sums, 0, 8, at(o)))


def y_kernel(sums, note, got, *refs):
    notes, half, pair, stage = refs[:3], *refs[3:]
    half[...] = sums[...] + joined(got, 0, 96)
    pair[0:32, :] = note[192:224, :]
    pair[32:64, :] = got[192:224, :]
    stage[...] = jnp.zeros_like(stage)
    for k in range(3):
        for dc in range(2):
            for j in range(TILES):
                q = j * 8 + 2 * (k + 1) + dc
                stage[dc * 12 + j : dc * 12 + j + 1, :] = half[q : q + 1, :]
        hi, lo = split(stage[...])
        notes[k][0:24, :] = hi
        notes[k][24:48, :] = lo
        notes[k][48:112, :] = pair[...]


def c_kernel(half, pair, got1, got2, got3, m0, msg, quarter, octet):
    quarter[...] = joined(got1, 0, 24) + joined(got2, 0, 24) + joined(got3, 0, 24)
    octet[0:64, :] = pair[...]
    for dy, g in ((1, got1), (2, got2), (3, got3)):
        octet[dy * 64 : dy * 64 + 64, :] = g[48:112, :]
    for dc in range(2):
        for j in range(TILES):
            r, q = dc * 12 + j, j * 8 + dc
            quarter[r : r + 1, :] = quarter[r : r + 1, :] + half[q : q + 1, :]
    hi, lo = split(quarter[12:24, :])
    msg[TAIL : TAIL + 12, :] = hi
    msg[TAIL + 16 : TAIL + 28, :] = lo
    msg[TAIL + 32 : TAIL + 288, :] = octet[...]


def total_kernel(gate, up, quarter, octet, got, out_g, out_u, total, sg, su, board, buf, obuf, sems, osems):
    here = where_am_i()
    copies = fetch(here, gate, up, [(0, 0, 0)], buf, sems)
    tail = got[TAIL : TAIL + 12, :].astype(F32) + got[TAIL + 16 : TAIL + 28, :].astype(F32)
    total[0:12, :] = quarter[0:12, :] + tail
    board[0:256, :] = octet[...]
    board[256:512, :] = got[TAIL + 32 : TAIL + 288, :]
    for i in range(HALF):
        sg[0:1, i * LANES : (i + 1) * LANES] = total[i : i + 1, :] / D_MODEL
        su[0:1, i * LANES : (i + 1) * LANES] = total[HALF + i : HALF + i + 1, :] / D_MODEL
    rows = pl.ds(pl.multiple_of(index(here, 0, 0, 0) * ROWS, ROWS), ROWS)
    back = []
    for h, out in enumerate((out_g, out_u)):
        copies[0][h].wait()
        for i in range(HALF):
            gain = D_MODEL / total[h * HALF + i : h * HALF + i + 1, :]
            cols = slice(i * LANES, (i + 1) * LANES)
            obuf[h, :, cols] = (buf[0, h, :, cols] * gain).astype(BF16)
        back.append(pltpu.make_async_copy(obuf.at[h], out.at[0, rows, :], osems.at[h]))
        back[-1].start()
    for b in back:
        b.wait()


def decode_kernel(offsets, total, *refs):
    n = len(offsets)
    msgs, outs, (buf, sems) = refs[:n], refs[n + 2 : n + 4], refs[n + 4 :]
    here = where_am_i()
    copies = []
    for k, (dz, dy, dc) in enumerate(offsets):
        rows = pl.ds(pl.multiple_of(index(here, dz, 4 - dy, dc) * ROWS, ROWS), ROWS)
        for h in range(2):
            for i in range(HALF):
                j = h * HALF + i
                unit = msgs[k][BODY + j : BODY + j + 1, :].astype(F32)
                gain = unit * (D_MODEL / SPAN) / total[j : j + 1, :]
                v = msgs[k][j * ROWS : (j + 1) * ROWS, :].astype(F32)
                w = (jnp.log2(jnp.abs(v)) + LOW) * gain
                buf[k, h, :, i * LANES : (i + 1) * LANES] = jnp.where(v < 0, -w, w).astype(BF16)
            copies.append(pltpu.make_async_copy(buf.at[k, h], outs[h].at[0, rows, :], sems.at[k, h]))
            copies[-1].start()
    for c in copies:
        c.wait()


def router_kernel(*refs):
    boards, out, buf = refs[:4], refs[4], refs[5]
    here = where_am_i()
    zl, x = lax.axis_index("zl"), lax.axis_index("x")
    for d in range(4):
        for b in range(2):
            col = pl.multiple_of(((zl ^ b) * 4 + (x + 8 - d - b) % 4) * 16, 16)
            for p in range(16):
                dc, dy, dz = p // 8, (p // 2) % 4, p % 2
                piece = boards[d][p * 32 + b * 16 : p * 32 + b * 16 + 16, :]
                buf[index(here, dz, 4 - dy, dc), pl.ds(col, 16), :] = piece.astype(F32)
    for s in range(16):
        out[s * ROWS : (s + 1) * ROWS, :] = buf[s].T.astype(BF16)


def shape(*dims, dtype=BF16):
    return jax.ShapeDtypeStruct(dims, dtype)


def local(*dims, dtype=BF16):
    return pltpu.VMEM(dims, dtype)


def message(extra=0):
    return local(TAIL + extra, LANES)


def near(value):
    return pltpu.with_memory_space_constraint(value, pltpu.VMEM)


def far(value):
    return pltpu.with_memory_space_constraint(value, pltpu.HBM)


def blocks(n):
    return [pltpu.VMEM((n, 2, ROWS, COLS), F32), pltpu.SemaphoreType.DMA((n, 2))]


def call(kernel, ins, outs, out_specs=None, **kw):
    def run(*args):
        return pl.pallas_call(
            kernel, in_specs=ins, out_specs=out_specs or [VMEM] * len(outs), out_shape=outs,
            compiler_params=pltpu.CompilerParams(vmem_limit_bytes=GRANT), **kw
        )(*args)
    return run


def moves(dz, dy, dc):
    return [
        (z * 8 + y * 2 + c, (z ^ dz) * 8 + ((y + dy) % 4) * 2 + (c ^ dc))
        for z in range(2) for y in range(4) for c in range(2)
    ]


def send(value, o):
    return lax.ppermute(value, SHARD, moves(*o))


GROUPS = [
    [(1, 0, 0), (0, 1, 1), (0, 3, 1), (1, 1, 0), (0, 3, 0), (1, 2, 0)],
    [(0, 1, 0), (1, 3, 0), (0, 2, 0), (0, 0, 1)],
    [(1, 0, 1), (1, 1, 1)],
    [(0, 2, 1), (1, 3, 1)],
    [(1, 2, 1)],
]


def step(gate, up, weight, gain):
    got = {}
    gate, up, weight, gain = (far(v) for v in (gate, up, weight.T, gain[None]))
    *first, sums, router = call(
        pre_kernel, [HBM] * 4, [message()] * len(PRE) + [local(192, LANES, dtype=F32), local(16, LANES)],
        scratch_shapes=[blocks(len(PRE))[0], pltpu.VMEM((16, LANES), F32), pltpu.VMEM((1, LANES), F32),
                        blocks(len(PRE))[1], pltpu.SemaphoreType.DMA((2,))],
    )(gate, up, weight, gain)
    for o, m in zip(PRE, first):
        got[o] = send(m, o)
    turn = [(z * 4 + x, (1 - z) * 4 + (x + 1) % 4) for z in range(2) for x in range(4)]
    other = near(lax.ppermute(router, ("zl", "x"), turn))
    *early, sums = call(
        mid_kernel, [HBM] * 2 + [VMEM], [message()] * len(MID) + [local(192, LANES, dtype=F32)],
        scratch_shapes=blocks(len(MID)),
    )(gate, up, sums)
    for o, m in zip(MID, early):
        got[o] = send(m, o)
    *rest, sums, note = call(
        main_kernel, [HBM] * 2 + [VMEM] * 3,
        [message()] * len(MAIN) + [local(192, LANES, dtype=F32), local(224, LANES)], scratch_shapes=blocks(len(MAIN)),
    )(gate, up, sums, router, other)
    turn = [(x * 2 + z, (x + 1) % 4 * 2 + 1 - z) for x in range(4) for z in range(2)]
    passed = near(lax.ppermute(note, ("x", "zh"), turn))
    got_note = near(lax.ppermute(passed, "x", [(i, (i + 3) % 4) for i in range(4)]))
    for o, m in zip(MAIN, rest):
        got[o] = send(m, o)
    *last, sums = call(
        more_kernel, [HBM] * 2 + [VMEM],
        [message()] * 3 + [message(288), local(96, LANES, dtype=F32)], scratch_shapes=blocks(len(MORE)),
    )(gate, up, sums)
    for o, m in zip(MORE[:3], last):
        got[o] = send(m, o)
    *notes, half, pair = call(
        y_kernel, [VMEM] * 3, [local(112, LANES)] * 3 + [local(96, LANES, dtype=F32), local(64, LANES)],
        scratch_shapes=[pltpu.VMEM((24, LANES), F32)],
    )(sums, note, got_note)
    got_y = []
    for dy, v in zip((1, 2, 3), notes):
        got_y.append(near(lax.ppermute(v, SHARD, moves(0, dy, 0))))
    across, quarter, octet = call(
        c_kernel, [VMEM] * 6, [message(288), local(24, LANES, dtype=F32), local(256, LANES)],
        input_output_aliases={5: 0},
    )(half, pair, *got_y, last[3])
    got[0, 0, 1] = near(send(across, (0, 0, 1)))
    whole = shape(1, D_MODEL, COLS)
    *outs, total, scale_gate, scale_up, board = call(
        total_kernel, [HBM] * 2 + [VMEM] * 3,
        [whole, whole, local(16, LANES, dtype=F32), shape(1, COLS, dtype=F32), shape(1, COLS, dtype=F32), local(512, LANES)],
        [HBM] * 2 + [VMEM] * 4,
        scratch_shapes=[blocks(1)[0], pltpu.VMEM((2, ROWS, COLS), BF16), blocks(1)[1], pltpu.SemaphoreType.DMA((2,))],
    )(gate, up, quarter, octet, got[0, 0, 1])
    boards = [board]
    for d in (1, 2, 3):
        boards.append(near(lax.ppermute(board, "x", [(i, (i + d) % 4) for i in range(4)])))
    for offsets in GROUPS:
        n = len(offsets)
        outs = call(
            functools.partial(decode_kernel, offsets), [VMEM] * (n + 1) + [HBM] * 2, [whole] * 2, [HBM] * 2,
            input_output_aliases={n + 1: 0, n + 2: 1},
            scratch_shapes=[pltpu.VMEM((n, 2, ROWS, COLS), BF16), pltpu.SemaphoreType.DMA((n, 2))],
        )(total, *(near(got[o]) for o in offsets), *outs)
    (serve_router,) = call(
        router_kernel, [VMEM] * 4, [shape(D_MODEL, LANES)], scratch_shapes=[pltpu.VMEM((16, LANES, LANES), F32)]
    )(*boards)
    return outs[0], outs[1], scale_gate, scale_up, serve_router


def solution(mesh):
    finer = Mesh(mesh.devices.reshape(2, 4, 2, 4, 2), ALL)
    expert = ("zl", "x")
    in_specs = (P(expert, SHARD, None), P(expert, SHARD, None), P(SHARD, expert), P(SHARD))
    out_specs = (P(ALL, None, None), P(ALL, None, None), P(ALL, None), P(ALL, None), P())
    return jax.shard_map(step, mesh=finer, in_specs=in_specs, out_specs=out_specs, check_vma=False)
```
